32 devices in a mesh: clip: 2 (over y), seq: 4 (over z), head: 4 (over x, core).
Axes of the slice: x: 2, y: 2, z: 4, core: 2. Of those that a mesh axis runs over, the one named last changes fastest.
Arguments:
- queries: bfloat16 [16, 4, 16, 3072], P(('clip', 'head'), 'seq'), parts along dimension 0, may hold values from -15 to 15
- attn_keys: bfloat16 [16, 4, 16, 3072], P(('clip', 'head'), 'seq'), parts along dimension 0, may hold values from -5 to 5
- attn_values: bfloat16 [16, 4, 16, 3072], P(('clip', 'head'), 'seq'), parts along dimension 0, may hold values from -5 to 5
- residual: bfloat16 [16, 4, 16, 5120], P(('clip', 'head'), 'seq'), parts along dimension 0, may hold values from -6 to 6
- out_weight: bfloat16 [3072, 5120], P('head', 'seq'), may hold values from -0.109375 to 0.109375
- out_gate: float32 [5120], replicated, may hold values from 0.3 to 3
- head_shift: float32 [5120], replicated, may hold values from -3 to 3
- head_scale: float32 [5120], replicated, may hold values from -1.5 to 1.5
- head_weight: bfloat16 [5120, 64], replicated, may hold values from -0.078125 to 0.078125
- head_bias: float32 [64], replicated, may hold values from -3 to 3
- conv_weight: bfloat16 [3, 3, 3, 16, 384], replicated, may hold values from -0.3125 to 0.3125
- conv_bias: float32 [384], replicated, may hold values from -3 to 3
- norm_gain: float32 [384], replicated, may hold values from 0.5 to 2
Outputs:
- hidden: bfloat16 [16, 4, 16, 5120], P(('clip', 'head'), 'seq'), parts along dimension 0
- features: bfloat16 [16, 8, 32, 384], P(('clip', 'head'), 'seq'), parts along dimension 0
The draws below stay inside these ranges and needn't reach their ends.
There are 2 independent parts, one for each index of `clip`. The reference program is written for one: setup_inputs(seed, part) draws one part's arguments, and reference() takes and returns one part's arrays. A program takes and returns all parts, laid end to end along the dimension named above; an argument that names none is the same for every part. Nothing has to cross between parts.
All inputs are finite; a program needn't handle non-finite values.
Results may differ from the reference program's by a relative error of at most 0.013.
Values may be sent and summed in bfloat16 or wider, within the bound.
No kernel may reach another device: no remote copies, remote signals or barrier semaphores. Data moves between devices by JAX's collectives and lax.ppermute only.
A program may use at most 128 MiB of HBM per device.

```python
import math
import jax
import jax.numpy as jnp
from jax import lax

D = 5120
HEAD_DIM = 128
HEADS = 24
LAT_CH = 16
VAE_CH = 384
WP = 16
F = 8
HP = 4
N_HEAD = 4


def draw_queries(key, part):
    count = F * HP * WP
    values = 3.0 * jnp.clip(jax.random.normal(jax.random.fold_in(key, 11), (count, HEADS, HEAD_DIM), jnp.float32), -5.0, 5.0)
    return values.reshape(F, HP, WP, HEADS * HEAD_DIM).astype(jnp.bfloat16)


def draw_attn_keys(key, part):
    count = F * HP * WP
    values = jnp.clip(jax.random.normal(jax.random.fold_in(key, 12), (count, HEADS, HEAD_DIM), jnp.float32), -5.0, 5.0)
    return values.reshape(F, HP, WP, HEADS * HEAD_DIM).astype(jnp.bfloat16)


def block_levels(own_key, dims, shards, low, top_value):
    def one(dim, shards_of):
        heights = jax.random.uniform(jax.random.fold_in(jax.random.fold_in(own_key, 6), dim), (shards_of,), jnp.float32, low / len(shards), top_value / len(shards))
        return jnp.repeat(jnp.exp(heights), dims[dim] // shards_of).reshape((-1,) + (1,) * (len(dims) - dim - 1))

    loudness = one(*shards[0])
    for cut in shards[1:]:
        loudness = loudness * one(*cut)
    return loudness


def centred(own_key, shape, deviation, reach, split=(), held_as=jnp.bfloat16):
    level = block_levels(own_key, shape, split, -0.22, 0.18) if split else 1.0
    entries = jax.random.normal(own_key, shape, jnp.float32) * deviation * level
    return jnp.minimum(jnp.maximum(entries, -reach), reach).astype(held_as)


def setup_inputs(seed: int = 0, part: int = 0) -> dict:
    key_list = jax.random.split(jax.random.key(seed), 14)
    own_keys = jax.random.split(jax.random.fold_in(key_list[13], part), 14)
    queries = draw_queries(jax.random.fold_in(jax.random.fold_in(key_list[13], part), 71), part)
    attn_keys = draw_attn_keys(jax.random.fold_in(jax.random.fold_in(key_list[13], part), 71), part)
    attn_values = centred(own_keys[2], (F, HP, WP, HEADS * HEAD_DIM), 1.0, 5.0, ((0, 4), (1, 4)))
    residual = centred(own_keys[3], (F, HP, WP, D), 1.0, 6.0, ((0, 4), (1, 4)))
    out_weight = centred(key_list[4], (HEADS * HEAD_DIM, D), (HEADS * HEAD_DIM) ** -0.5, 0.109375, ((0, 4), (1, 4)))
    out_gate = jnp.clip(jnp.exp(jax.random.uniform(key_list[5], (D,), jnp.float32, math.log(0.3), math.log(3.0))), 0.3, 3.0)
    head_shift = centred(key_list[6], (D,), 0.5, 3.0, (), jnp.float32)
    head_scale = centred(key_list[7], (D,), 0.3, 1.5, (), jnp.float32)
    head_weight = centred(key_list[8], (D, 4 * LAT_CH), D ** -0.5, 0.078125)
    head_bias = centred(key_list[9], (4 * LAT_CH,), 0.5, 3.0, (), jnp.float32)
    conv_weight = centred(key_list[10], (3, 3, 3, LAT_CH, VAE_CH), (27 * LAT_CH) ** -0.5, 0.3125)
    conv_bias = centred(key_list[11], (VAE_CH,), 0.5, 3.0, (), jnp.float32)
    norm_gain = jnp.clip(jnp.exp(jax.random.uniform(key_list[12], (VAE_CH,), jnp.float32, math.log(0.5), math.log(2.0))), 0.5, 2.0)
    return {"queries": queries, "attn_keys": attn_keys, "attn_values": attn_values, "residual": residual, "out_weight": out_weight, "out_gate": out_gate, "head_shift": head_shift, "head_scale": head_scale, "head_weight": head_weight, "head_bias": head_bias, "conv_weight": conv_weight, "conv_bias": conv_bias, "norm_gain": norm_gain}


def head_latent(hidden, head_shift, head_scale, head_weight, head_bias):
    values = hidden.astype(jnp.float32)
    center = values - lax.optimization_barrier(jnp.mean(values, -1, keepdims=True))
    spread = lax.optimization_barrier(jnp.mean(center * center, -1, keepdims=True))
    normed = (center * lax.rsqrt(spread + 1e-06) * (1.0 + head_scale) + head_shift).astype(jnp.bfloat16)
    flat = normed.reshape(-1, normed.shape[-1])
    latent = (jnp.dot(flat, head_weight, preferred_element_type=jnp.float32) + head_bias).astype(jnp.bfloat16)
    frames, height, breadth = (hidden.shape[0], hidden.shape[1], hidden.shape[2])
    channels = head_weight.shape[1] // 4
    patches = latent.reshape(frames, height, breadth, 2, 2, channels).transpose(0, 1, 3, 2, 4, 5)
    return patches.reshape(frames, height * 2, breadth * 2, channels)

def convolve(padded, frames, conv_weight, conv_bias, norm_gain):
    height = padded.shape[1] - 2
    breadth = padded.shape[2] - 2
    stacked = jnp.concatenate([padded[time_off:time_off + frames, row_off:row_off + height, col_off:col_off + breadth] for time_off in range(3) for row_off in range(3) for col_off in range(3)], -1)
    kernel = conv_weight.reshape(-1, conv_weight.shape[-1])
    linear = jnp.dot(stacked.reshape(-1, stacked.shape[-1]), kernel, preferred_element_type=jnp.float32) + conv_bias
    normed = linear * lax.rsqrt(lax.optimization_barrier(jnp.mean(linear * linear, -1, keepdims=True)) + 1e-06) * norm_gain
    return jax.nn.silu(normed).astype(jnp.bfloat16).reshape(frames, height, breadth, -1)

def one_head(triple):
    query_one, key_one, value_one = triple
    scores = jnp.dot(query_one, key_one.T, preferred_element_type=jnp.float32) * query_one.shape[-1] ** (-0.5)
    peak = lax.optimization_barrier(jnp.max(scores, -1, keepdims=True))
    weights = jnp.exp(scores - peak)
    denominator = lax.optimization_barrier(jnp.sum(weights, -1, keepdims=True))
    product = jnp.dot(weights.astype(jnp.bfloat16), value_one, preferred_element_type=jnp.float32)
    return (product / denominator).astype(jnp.bfloat16)

def add_group(running_sum, pair):
    term = jnp.dot(pair[0], pair[1], preferred_element_type=jnp.float32).astype(jnp.bfloat16)
    term = lax.optimization_barrier(term).astype(jnp.float32)
    return (running_sum + term, None)

def reference(queries, attn_keys, attn_values, residual, out_weight, out_gate, head_shift, head_scale, head_weight, head_bias, conv_weight, conv_bias, norm_gain):
    count = F * HP * WP
    query_heads = queries.reshape(count, HEADS, HEAD_DIM).transpose(1, 0, 2)
    key_heads = attn_keys.reshape(count, HEADS, HEAD_DIM).transpose(1, 0, 2)
    value_heads = attn_values.reshape(count, HEADS, HEAD_DIM).transpose(1, 0, 2)
    attended = lax.map(one_head, (query_heads, key_heads, value_heads))
    attended = attended.transpose(1, 0, 2).reshape(count, HEADS * HEAD_DIM)
    group_width = HEADS // N_HEAD * HEAD_DIM
    groups_in = attended.reshape(count, N_HEAD, group_width).transpose(1, 0, 2)
    weights_in = out_weight.reshape(N_HEAD, group_width, D)
    projected, _ = lax.scan(add_group, jnp.zeros((count, D), jnp.float32), (groups_in, weights_in))
    projected = projected.reshape(F, HP, WP, D)
    hidden = (residual.astype(jnp.float32) + out_gate * projected).astype(jnp.bfloat16)
    video = head_latent(hidden, head_shift, head_scale, head_weight, head_bias)
    padded = jnp.pad(video, ((2, 0), (1, 1), (1, 1), (0, 0)))
    features = convolve(padded, F, conv_weight, conv_bias, norm_gain)
    return (hidden, features)
```

```python
import jax
import jax.numpy as jnp
from jax import lax
from jax.experimental import pallas as pl
from jax.experimental.pallas import tpu as pltpu
from jax.sharding import PartitionSpec as P

HEAD_DIM = 128


def from_behind(value, axis, steps):
    count = lax.axis_size(axis)
    first, last = (max(0, -steps), min(count, count - steps))
    return lax.ppermute(value, axis, [(source, source + steps) for source in range(first, last)])


def padded_2(x, sides, width):
    for axis, dim in sides:
        peers, length = (lax.axis_size(axis), x.shape[dim])
        up = [(i, (i + 1) % peers) for i in range(peers - 1)]
        down = [(j, i) for i, j in up]
        last = lax.slice_in_dim(x, length - width, length, axis=dim)
        first = lax.slice_in_dim(x, 0, width, axis=dim)
        before = lax.ppermute(last, axis, up)
        after = lax.ppermute(first, axis, down)
        x = jnp.concatenate([before, x, after], axis=dim)
    return x


def head_latent(hidden, head_shift, head_scale, head_weight, head_bias):
    values = hidden.astype(jnp.float32)
    center = values - jnp.mean(values, -1, keepdims=True)
    spread = jnp.mean(center * center, -1, keepdims=True)
    normed = (center * lax.rsqrt(spread + 1e-06) * (1.0 + head_scale) + head_shift).astype(
        jnp.bfloat16
    )
    flat = normed.reshape(-1, normed.shape[-1])
    latent = (jnp.dot(flat, head_weight, preferred_element_type=jnp.float32) + head_bias).astype(
        jnp.bfloat16
    )
    frames, height, breadth = (hidden.shape[0], hidden.shape[1], hidden.shape[2])
    channels = head_weight.shape[1] // 4
    patches = latent.reshape(frames, height, breadth, 2, 2, channels).transpose(0, 1, 3, 2, 4, 5)
    return patches.reshape(frames, height * 2, breadth * 2, channels)


def convolve(padded, frames, conv_weight, conv_bias, norm_gain):
    height = padded.shape[1] - 2
    breadth = padded.shape[2] - 2
    stacked = jnp.concatenate(
        [
            padded[
                time_off : time_off + frames,
                row_off : row_off + height,
                col_off : col_off + breadth,
            ]
            for time_off in range(3)
            for row_off in range(3)
            for col_off in range(3)
        ],
        -1,
    )
    kernel = conv_weight.reshape(-1, conv_weight.shape[-1])
    linear = (
        jnp.dot(stacked.reshape(-1, stacked.shape[-1]), kernel, preferred_element_type=jnp.float32)
        + conv_bias
    )
    normed = linear * lax.rsqrt(jnp.mean(linear * linear, -1, keepdims=True) + 1e-06) * norm_gain
    return jax.nn.silu(normed).astype(jnp.bfloat16).reshape(frames, height, breadth, -1)


def attend_block(carried, block_keys, block_values, query_heads):
    running, denominator, weighted = carried
    scores = jnp.einsum("hqd,khd->hqk", query_heads, block_keys, preferred_element_type=jnp.float32)
    scores = scores * query_heads.shape[-1] ** (-0.5)
    newmax = jnp.maximum(running, jnp.max(scores, -1))
    factor = jnp.exp(running - newmax)
    weights = jnp.exp(scores - newmax[..., None])
    denominator = denominator * factor + jnp.sum(weights, -1)
    product = jnp.einsum(
        "hqk,khd->hqd",
        weights.astype(jnp.bfloat16),
        block_values,
        preferred_element_type=jnp.float32,
    )
    weighted = weighted * factor[..., None] + product
    return (newmax, denominator, weighted)


def fold_pieces(query_heads, carried, pieces):
    key_piece, value_piece = pieces
    frames, height, breadth = (key_piece.shape[0], key_piece.shape[1], key_piece.shape[2])
    heads_here, head_width = (query_heads.shape[0], query_heads.shape[2])
    group_rows = 4

    def regroup(one_piece):
        shaped = one_piece.reshape(
            frames, height // group_rows, group_rows, breadth, heads_here, head_width
        )
        shaped = shaped.transpose(1, 0, 2, 3, 4, 5)
        return shaped.reshape(
            height // group_rows, frames * group_rows * breadth, heads_here, head_width
        )

    def advance(inner, blocks):
        return (attend_block(inner, blocks[0], blocks[1], query_heads), None)

    carried, _ = lax.scan(advance, carried, (regroup(key_piece), regroup(value_piece)))
    return carried


def general_path(
    queries,
    attn_keys,
    attn_values,
    residual,
    out_weight,
    out_gate,
    head_shift,
    head_scale,
    head_weight,
    head_bias,
    conv_weight,
    conv_bias,
    norm_gain,
):
    head_count = lax.axis_size("head")
    frames_dev = queries.shape[0]
    group_width = queries.shape[3] // head_count
    head_width = HEAD_DIM
    heads_here = group_width // head_width
    local_queries, local_keys, local_values = (
        lax.all_to_all(queries, "head", split_axis=3, concat_axis=0, tiled=True),
        lax.all_to_all(attn_keys, "head", split_axis=3, concat_axis=0, tiled=True),
        lax.all_to_all(attn_values, "head", split_axis=3, concat_axis=0, tiled=True),
    )
    frames_all, height, breadth = (
        local_queries.shape[0],
        local_queries.shape[1],
        local_queries.shape[2],
    )
    count = frames_all * height * breadth
    query_heads = local_queries.reshape(count, heads_here, head_width).transpose(1, 0, 2)
    initial = (
        jnp.full((heads_here, count), -1e30, jnp.float32),
        jnp.zeros((heads_here, count), jnp.float32),
        jnp.zeros((heads_here, count, head_width), jnp.float32),
    )
    carried = fold_pieces(
        query_heads,
        initial,
        (
            lax.all_gather(local_keys, "seq", axis=1, tiled=True),
            lax.all_gather(local_values, "seq", axis=1, tiled=True),
        ),
    )
    running, denominator, weighted = carried
    attended = (weighted / denominator[..., None]).astype(jnp.bfloat16)
    attended = attended.transpose(1, 0, 2).reshape(count, group_width)
    partial_value = jnp.dot(
        attended,
        lax.all_gather(out_weight, "seq", axis=1, tiled=True),
        preferred_element_type=jnp.float32,
    )
    partial_value = partial_value.reshape(frames_all, height, breadth, partial_value.shape[-1])
    owned = lax.psum_scatter(
        partial_value.astype(jnp.bfloat16), "head", scatter_dimension=0, tiled=True
    ).astype(jnp.float32)
    hidden = (residual.astype(jnp.float32) + out_gate * owned).astype(jnp.bfloat16)
    own_video = head_latent(hidden, head_shift, head_scale, head_weight, head_bias)
    earlier = from_behind(own_video, "head", 1)
    video = jnp.concatenate([earlier, own_video], 0)
    extended = padded_2(video, (("seq", 1),), 1)
    padded = jnp.pad(extended, ((0, 0), (0, 0), (1, 1), (0, 0)))
    features = convolve(padded, frames_dev, conv_weight, conv_bias, norm_gain)
    return (hidden, features)


def pack_heads(queries, keys, values, seq_count, head_count):
    tokens, width = queries.shape
    group = width // HEAD_DIM // head_count
    whole, shared = divmod(group, seq_count)
    slots = whole + (shared > 0)

    def heads_of(seq):
        owned = [seq * whole + i for i in range(whole)]
        if shared:
            owned.append(whole * seq_count + seq // (seq_count // shared))
        return owned

    def kernel(q_ref, k_ref, v_ref, out_ref):
        for seq in range(seq_count):
            for head in range(head_count):
                for slot, local in enumerate(heads_of(seq)):
                    col = (head * group + local) * HEAD_DIM
                    for part, ref in enumerate((q_ref, k_ref, v_ref)):
                        to = (slot * 3 + part) * HEAD_DIM
                        out_ref[seq * head_count + head, :, to : to + HEAD_DIM] = ref[
                            :, col : col + HEAD_DIM
                        ]

    return pl.pallas_call(
        kernel,
        out_shape=jax.ShapeDtypeStruct(
            (seq_count * head_count, tokens, slots * 3 * HEAD_DIM), queries.dtype
        ),
        name="pack_heads",
    )(queries, keys, values)


def attend_kernel_call(packed, seq_count, head_count, group):
    tokens = packed.shape[1]
    whole, shared = divmod(group, seq_count)
    sharers = seq_count // shared if shared else 1
    row = head_count * tokens
    total = seq_count * row
    part_rows = seq_count // sharers
    out_blocks = whole * seq_count + (part_rows if shared else 0)
    part = (lax.axis_index("seq") % sharers).astype(jnp.int32).reshape(1)

    def kernel(part_ref, x_ref, out_ref):
        def one(slot, first, rows_of_seq, base):
            at = slot * 3 * HEAD_DIM
            count = rows_of_seq * head_count
            q = x_ref[pl.ds(first, count), :, at : at + HEAD_DIM]
            q = q.reshape(count * tokens, HEAD_DIM)
            k = x_ref[:, :, at + HEAD_DIM : at + 2 * HEAD_DIM].reshape(total, HEAD_DIM)
            v = x_ref[:, :, at + 2 * HEAD_DIM : at + 3 * HEAD_DIM].reshape(total, HEAD_DIM)
            scores = lax.dot_general(
                q, k, (((1,), (1,)), ((), ())), preferred_element_type=jnp.float32
            )
            scores = scores * HEAD_DIM ** (-0.5)
            weights = jnp.exp(scores - jnp.max(scores, -1, keepdims=True))
            denominator = jnp.sum(weights, -1, keepdims=True)
            product = jnp.dot(weights.astype(jnp.bfloat16), v, preferred_element_type=jnp.float32)
            result = (product / denominator).astype(jnp.bfloat16)
            for seq in range(rows_of_seq):
                for head in range(head_count):
                    at_row = (seq * head_count + head) * tokens
                    to = (base + seq) * tokens
                    out_ref[head, to : to + tokens, :] = result[at_row : at_row + tokens, :]

        for slot in range(whole):
            one(slot, 0, seq_count, slot * seq_count)
        if shared:
            one(whole, part_ref[0] * part_rows * head_count, part_rows, whole * seq_count)

    return pl.pallas_call(
        kernel,
        in_specs=[
            pl.BlockSpec(memory_space=pltpu.SMEM),
            pl.BlockSpec(memory_space=pltpu.VMEM),
        ],
        out_shape=jax.ShapeDtypeStruct(
            (head_count, out_blocks * tokens, HEAD_DIM), jnp.bfloat16
        ),
        name="attend",
    )(part, packed)


def project_kernel_call(gathered, weights, seq_count, head_count, group, tokens):
    whole, shared = divmod(group, seq_count)
    sharers = seq_count // shared if shared else 1
    part_rows = seq_count // sharers
    rows = seq_count * tokens
    width = weights[0].shape[1]
    block = width // 5 if width % 640 == 0 else width
    me = lax.axis_index("head").astype(jnp.int32).reshape(1)

    def kernel(me_ref, x_ref, *refs):
        w_refs, out_ref, a_ref = (refs[:-2], refs[-2], refs[-1])

        @pl.when(pl.program_id(0) == 0)
        def _():
            for seq in range(seq_count):
                for head in range(head_count):
                    for slot in range(whole):
                        col = (seq * whole + slot) * HEAD_DIM
                        a_ref[head, :, col : col + HEAD_DIM] = x_ref[
                            seq, head, slot * rows : (slot + 1) * rows, :
                        ]
                    if shared:
                        col = (whole * seq_count + seq // sharers) * HEAD_DIM
                        to = (seq % sharers) * part_rows * tokens
                        a_ref[head, to : to + part_rows * tokens, col : col + HEAD_DIM] = x_ref[
                            seq, head, whole * rows : whole * rows + part_rows * tokens, :
                        ]

        total = None
        for offset, w_ref in enumerate(w_refs):
            term = jnp.dot(
                a_ref[me_ref[0] ^ offset], w_ref[...], preferred_element_type=jnp.float32
            )
            total = term if total is None else total + term
        total = total.astype(jnp.bfloat16)
        for seq in range(seq_count):
            out_ref[seq] = total[seq * tokens : (seq + 1) * tokens]

    return pl.pallas_call(
        kernel,
        grid=(width // block,),
        in_specs=[
            pl.BlockSpec(memory_space=pltpu.SMEM),
            pl.BlockSpec(gathered.shape, lambda i: (0, 0, 0, 0)),
        ]
        + [pl.BlockSpec((w.shape[0], block), lambda i: (0, i)) for w in weights],
        out_specs=pl.BlockSpec((seq_count, tokens, block), lambda i: (0, 0, i)),
        out_shape=jax.ShapeDtypeStruct((seq_count, tokens, width), jnp.bfloat16),
        scratch_shapes=[pltpu.VMEM((head_count, rows, group * HEAD_DIM), jnp.bfloat16)],
        name="project",
    )(me, gathered, *weights)


def finish_kernel_call(columns, residual, gate, shift, scale, head_weight, head_bias):
    parts, tokens, width = columns.shape
    model = parts * width

    def kernel(y_ref, r_ref, g_ref, sh_ref, sc_ref, w_ref, b_ref, h_ref, p_ref):
        total = jnp.zeros((tokens, 1), jnp.float32)
        for i in range(parts):
            at = slice(i * width, (i + 1) * width)
            hidden = (
                r_ref[:, at].astype(jnp.float32) + g_ref[:, at] * y_ref[i].astype(jnp.float32)
            ).astype(jnp.bfloat16)
            h_ref[:, at] = hidden
            total = total + jnp.sum(hidden.astype(jnp.float32), -1, keepdims=True)
        mean = total / model
        square = jnp.zeros((tokens, 1), jnp.float32)
        for i in range(parts):
            center = h_ref[:, i * width : (i + 1) * width].astype(jnp.float32) - mean
            square = square + jnp.sum(center * center, -1, keepdims=True)
        inverse = lax.rsqrt(square / model + 1e-06)
        latent = jnp.zeros((tokens, w_ref.shape[1]), jnp.float32)
        for i in range(parts):
            at = slice(i * width, (i + 1) * width)
            center = h_ref[:, at].astype(jnp.float32) - mean
            normed = (center * inverse * (1.0 + sc_ref[:, at]) + sh_ref[:, at]).astype(jnp.bfloat16)
            latent = latent + jnp.dot(normed, w_ref[at, :], preferred_element_type=jnp.float32)
        p_ref[...] = (latent + b_ref[...]).astype(jnp.bfloat16)

    return pl.pallas_call(
        kernel,
        out_shape=(
            jax.ShapeDtypeStruct((tokens, model), jnp.bfloat16),
            jax.ShapeDtypeStruct((tokens, head_weight.shape[1]), jnp.bfloat16),
        ),
        name="finish",
    )(
        columns,
        residual,
        gate.reshape(1, -1),
        shift.reshape(1, -1),
        scale.reshape(1, -1),
        head_weight,
        head_bias.reshape(1, -1),
    )


def neighbour(value, seq_step, head_step):
    seq_count, head_count = (lax.axis_size("seq"), lax.axis_size("head"))
    pairs = []
    for seq in range(seq_count):
        for head in range(head_count):
            to_seq, to_head = (seq + seq_step, head + head_step)
            if 0 <= to_seq < seq_count and 0 <= to_head < head_count:
                pairs.append((seq * head_count + head, to_seq * head_count + to_head))
    return lax.ppermute(value, ("seq", "head"), pairs)


def all_groups(weight, head_count):
    held = {0: weight}
    bit = head_count // 2
    while bit:
        pairs = [(i, i ^ bit) for i in range(head_count)]
        held.update({j ^ bit: lax.ppermute(w, "head", pairs) for j, w in list(held.items())})
        bit //= 2
    return [held[j] for j in range(head_count)]


def on_device(
    queries,
    attn_keys,
    attn_values,
    residual,
    out_weight,
    out_gate,
    head_shift,
    head_scale,
    head_weight,
    head_bias,
    conv_weight,
    conv_bias,
    norm_gain,
):
    head_count, seq_count = (lax.axis_size("head"), lax.axis_size("seq"))
    frames, height, breadth, width = queries.shape
    group = width // HEAD_DIM // head_count
    shared = group % seq_count
    tokens = frames * height * breadth
    fits = (
        group >= seq_count
        and (shared == 0 or seq_count % shared == 0)
        and head_count & (head_count - 1) == 0
        and height == 1
        and tokens % 16 == 0
        and frames >= 2
    )
    if not fits:
        return general_path(
            queries,
            attn_keys,
            attn_values,
            residual,
            out_weight,
            out_gate,
            head_shift,
            head_scale,
            head_weight,
            head_bias,
            conv_weight,
            conv_bias,
            norm_gain,
        )
    weights = all_groups(out_weight, head_count)
    packed = pack_heads(
        queries.reshape(tokens, width),
        attn_keys.reshape(tokens, width),
        attn_values.reshape(tokens, width),
        seq_count,
        head_count,
    )
    packed = lax.all_to_all(packed, ("seq", "head"), split_axis=0, concat_axis=0, tiled=True)
    attended = attend_kernel_call(packed, seq_count, head_count, group)
    attended = lax.all_to_all(attended, "head", split_axis=0, concat_axis=0, tiled=True)
    gathered = lax.all_gather(attended, "seq", axis=0, tiled=False)
    columns = project_kernel_call(gathered, weights, seq_count, head_count, group, tokens)
    columns = lax.all_to_all(columns, "seq", split_axis=0, concat_axis=0, tiled=True)
    hidden, latent = finish_kernel_call(
        columns,
        residual.reshape(tokens, -1),
        out_gate,
        head_shift,
        head_scale,
        head_weight,
        head_bias,
    )
    before = [neighbour(latent, step, 1) for step in (1, 0, -1)]
    now = [neighbour(latent, 1, 0), latent, neighbour(latent, -1, 0)]
    channels = latent.shape[1] // 4
    grid = jnp.stack([jnp.stack(before), jnp.stack(now)]).reshape(
        2, 3, frames, breadth, 2, 2, channels
    )
    video = grid.transpose(0, 2, 1, 4, 3, 5, 6).reshape(2 * frames, 6, 2 * breadth, channels)
    video = video[frames - 2 :, 1:5]
    padded = jnp.pad(video, ((0, 0), (0, 0), (1, 1), (0, 0)))
    features = convolve(padded, frames, conv_weight, conv_bias, norm_gain)
    return (hidden.reshape(residual.shape), features)


def solution(mesh):
    return jax.shard_map(
        on_device,
        mesh=mesh,
        in_specs=(
            P(("clip", "head"), "seq", None, None),
            P(("clip", "head"), "seq", None, None),
            P(("clip", "head"), "seq", None, None),
            P(("clip", "head"), "seq", None, None),
            P("head", "seq"),
            P(),
            P(),
            P(),
            P(),
            P(),
            P(),
            P(),
            P(),
        ),
        out_specs=(P(("clip", "head"), "seq", None, None), P(("clip", "head"), "seq", None, None)),
        check_vma=False,
    )
```

```python
import jax
import jax.numpy as jnp
from jax import lax
from jax.experimental import pallas as pl
from jax.experimental.pallas import tpu as pltpu
from jax.sharding import PartitionSpec as P

HEAD_DIM = 128


def from_behind(value, axis, steps):
    count = lax.axis_size(axis)
    first, last = (max(0, -steps), min(count, count - steps))
    return lax.ppermute(value, axis, [(source, source + steps) for source in range(first, last)])


def padded_2(x, sides, width):
    for axis, dim in sides:
        peers, length = (lax.axis_size(axis), x.shape[dim])
        up = [(i, (i + 1) % peers) for i in range(peers - 1)]
        down = [(j, i) for i, j in up]
        last = lax.slice_in_dim(x, length - width, length, axis=dim)
        first = lax.slice_in_dim(x, 0, width, axis=dim)
        before = lax.ppermute(last, axis, up)
        after = lax.ppermute(first, axis, down)
        x = jnp.concatenate([before, x, after], axis=dim)
    return x


def head_latent(hidden, head_shift, head_scale, head_weight, head_bias):
    values = hidden.astype(jnp.float32)
    center = values - jnp.mean(values, -1, keepdims=True)
    spread = jnp.mean(center * center, -1, keepdims=True)
    normed = (center * lax.rsqrt(spread + 1e-06) * (1.0 + head_scale) + head_shift).astype(
        jnp.bfloat16
    )
    flat = normed.reshape(-1, normed.shape[-1])
    latent = (jnp.dot(flat, head_weight, preferred_element_type=jnp.float32) + head_bias).astype(
        jnp.bfloat16
    )
    frames, height, breadth = (hidden.shape[0], hidden.shape[1], hidden.shape[2])
    channels = head_weight.shape[1] // 4
    patches = latent.reshape(frames, height, breadth, 2, 2, channels).transpose(0, 1, 3, 2, 4, 5)
    return patches.reshape(frames, height * 2, breadth * 2, channels)


def convolve(padded, frames, conv_weight, conv_bias, norm_gain):
    height = padded.shape[1] - 2
    breadth = padded.shape[2] - 2
    stacked = jnp.concatenate(
        [
            padded[
                time_off : time_off + frames,
                row_off : row_off + height,
                col_off : col_off + breadth,
            ]
            for time_off in range(3)
            for row_off in range(3)
            for col_off in range(3)
        ],
        -1,
    )
    kernel = conv_weight.reshape(-1, conv_weight.shape[-1])
    linear = (
        jnp.dot(stacked.reshape(-1, stacked.shape[-1]), kernel, preferred_element_type=jnp.float32)
        + conv_bias
    )
    normed = linear * lax.rsqrt(jnp.mean(linear * linear, -1, keepdims=True) + 1e-06) * norm_gain
    return jax.nn.silu(normed).astype(jnp.bfloat16).reshape(frames, height, breadth, -1)


def attend_block(carried, block_keys, block_values, query_heads):
    running, denominator, weighted = carried
    scores = jnp.einsum("hqd,khd->hqk", query_heads, block_keys, preferred_element_type=jnp.float32)
    scores = scores * query_heads.shape[-1] ** (-0.5)
    newmax = jnp.maximum(running, jnp.max(scores, -1))
    factor = jnp.exp(running - newmax)
    weights = jnp.exp(scores - newmax[..., None])
    denominator = denominator * factor + jnp.sum(weights, -1)
    product = jnp.einsum(
        "hqk,khd->hqd",
        weights.astype(jnp.bfloat16),
        block_values,
        preferred_element_type=jnp.float32,
    )
    weighted = weighted * factor[..., None] + product
    return (newmax, denominator, weighted)


def fold_pieces(query_heads, carried, pieces):
    key_piece, value_piece = pieces
    frames, height, breadth = (key_piece.shape[0], key_piece.shape[1], key_piece.shape[2])
    heads_here, head_width = (query_heads.shape[0], query_heads.shape[2])
    group_rows = 4

    def regroup(one_piece):
        shaped = one_piece.reshape(
            frames, height // group_rows, group_rows, breadth, heads_here, head_width
        )
        shaped = shaped.transpose(1, 0, 2, 3, 4, 5)
        return shaped.reshape(
            height // group_rows, frames * group_rows * breadth, heads_here, head_width
        )

    def advance(inner, blocks):
        return (attend_block(inner, blocks[0], blocks[1], query_heads), None)

    carried, _ = lax.scan(advance, carried, (regroup(key_piece), regroup(value_piece)))
    return carried


def general_path(
    queries,
    attn_keys,
    attn_values,
    residual,
    out_weight,
    out_gate,
    head_shift,
    head_scale,
    head_weight,
    head_bias,
    conv_weight,
    conv_bias,
    norm_gain,
):
    head_count = lax.axis_size("head")
    frames_dev = queries.shape[0]
    group_width = queries.shape[3] // head_count
    head_width = HEAD_DIM
    heads_here = group_width // head_width
    local_queries, local_keys, local_values = (
        lax.all_to_all(queries, "head", split_axis=3, concat_axis=0, tiled=True),
        lax.all_to_all(attn_keys, "head", split_axis=3, concat_axis=0, tiled=True),
        lax.all_to_all(attn_values, "head", split_axis=3, concat_axis=0, tiled=True),
    )
    frames_all, height, breadth = (
        local_queries.shape[0],
        local_queries.shape[1],
        local_queries.shape[2],
    )
    count = frames_all * height * breadth
    query_heads = local_queries.reshape(count, heads_here, head_width).transpose(1, 0, 2)
    initial = (
        jnp.full((heads_here, count), -1e30, jnp.float32),
        jnp.zeros((heads_here, count), jnp.float32),
        jnp.zeros((heads_here, count, head_width), jnp.float32),
    )
    carried = fold_pieces(
        query_heads,
        initial,
        (
            lax.all_gather(local_keys, "seq", axis=1, tiled=True),
            lax.all_gather(local_values, "seq", axis=1, tiled=True),
        ),
    )
    running, denominator, weighted = carried
    attended = (weighted / denominator[..., None]).astype(jnp.bfloat16)
    attended = attended.transpose(1, 0, 2).reshape(count, group_width)
    partial_value = jnp.dot(
        attended,
        lax.all_gather(out_weight, "seq", axis=1, tiled=True),
        preferred_element_type=jnp.float32,
    )
    partial_value = partial_value.reshape(frames_all, height, breadth, partial_value.shape[-1])
    owned = lax.psum_scatter(
        partial_value.astype(jnp.bfloat16), "head", scatter_dimension=0, tiled=True
    ).astype(jnp.float32)
    hidden = (residual.astype(jnp.float32) + out_gate * owned).astype(jnp.bfloat16)
    own_video = head_latent(hidden, head_shift, head_scale, head_weight, head_bias)
    earlier = from_behind(own_video, "head", 1)
    video = jnp.concatenate([earlier, own_video], 0)
    extended = padded_2(video, (("seq", 1),), 1)
    padded = jnp.pad(extended, ((0, 0), (0, 0), (1, 1), (0, 0)))
    features = convolve(padded, frames_dev, conv_weight, conv_bias, norm_gain)
    return (hidden, features)


def pack_heads(queries, keys, values, seq_count, head_count):
    tokens, width = queries.shape
    group = width // HEAD_DIM // head_count
    whole, shared = divmod(group, seq_count)
    slots = whole + (shared > 0)

    def heads_of(seq):
        owned = [seq * whole + i for i in range(whole)]
        if shared:
            owned.append(whole * seq_count + seq // (seq_count // shared))
        return owned

    def kernel(q_ref, k_ref, v_ref, out_ref):
        for seq in range(seq_count):
            for head in range(head_count):
                for slot, local in enumerate(heads_of(seq)):
                    col = (head * group + local) * HEAD_DIM
                    for part, ref in enumerate((q_ref, k_ref, v_ref)):
                        to = (slot * 3 + part) * HEAD_DIM
                        out_ref[seq * head_count + head, :, to : to + HEAD_DIM] = ref[
                            :, col : col + HEAD_DIM
                        ]

    return pl.pallas_call(
        kernel,
        out_shape=jax.ShapeDtypeStruct(
            (seq_count * head_count, tokens, slots * 3 * HEAD_DIM), queries.dtype
        ),
        name="pack_heads",
    )(queries, keys, values)


def attend_kernel_call(packed, seq_count, head_count, group):
    tokens = packed.shape[1]
    whole, shared = divmod(group, seq_count)
    sharers = seq_count // shared if shared else 1
    row = head_count * tokens
    total = seq_count * row
    part_rows = seq_count // sharers
    out_blocks = whole * seq_count + (part_rows if shared else 0)
    outer = head_count // 2
    place = jnp.stack([lax.axis_index("seq") % sharers, lax.axis_index("head") % 2])

    def kernel(place_ref, x_ref, keep_ref, send_ref, result_ref):
        def one(slot, first, rows_of_seq, base):
            at = slot * 3 * HEAD_DIM
            count = rows_of_seq * head_count
            q = x_ref[pl.ds(first, count), :, at : at + HEAD_DIM]
            q = q.reshape(count * tokens, HEAD_DIM)
            k = x_ref[:, :, at + HEAD_DIM : at + 2 * HEAD_DIM].reshape(total, HEAD_DIM)
            v = x_ref[:, :, at + 2 * HEAD_DIM : at + 3 * HEAD_DIM].reshape(total, HEAD_DIM)
            scores = lax.dot_general(
                q, k, (((1,), (1,)), ((), ())), preferred_element_type=jnp.float32
            )
            scores = scores * HEAD_DIM ** (-0.5)
            weights = jnp.exp(scores - jnp.max(scores, -1, keepdims=True))
            denominator = jnp.sum(weights, -1, keepdims=True)
            product = jnp.dot(weights.astype(jnp.bfloat16), v, preferred_element_type=jnp.float32)
            result = (product / denominator).astype(jnp.bfloat16)
            result_ref[0:count] = result.reshape(count, tokens, HEAD_DIM)
            for seq in range(rows_of_seq):
                for far in range(outer):
                    to = (base + seq) * tokens
                    mine = seq * head_count + far * 2
                    keep_ref[far, to : to + tokens, :] = result_ref[mine + place_ref[1]]
                    send_ref[far, to : to + tokens, :] = result_ref[mine + 1 - place_ref[1]]

        for slot in range(whole):
            one(slot, 0, seq_count, slot * seq_count)
        if shared:
            one(whole, place_ref[0] * part_rows * head_count, part_rows, whole * seq_count)

    half = jax.ShapeDtypeStruct((outer, out_blocks * tokens, HEAD_DIM), jnp.bfloat16)
    return pl.pallas_call(
        kernel,
        in_specs=[
            pl.BlockSpec(memory_space=pltpu.SMEM),
            pl.BlockSpec(memory_space=pltpu.VMEM),
        ],
        out_shape=(half, half),
        scratch_shapes=[pltpu.VMEM((seq_count * head_count, tokens, HEAD_DIM), jnp.bfloat16)],
        name="attend",
    )(place.astype(jnp.int32), packed)


def project_kernel_call(gathered, weights, seq_count, group, tokens):
    whole, shared = divmod(group, seq_count)
    sharers = seq_count // shared if shared else 1
    part_rows = seq_count // sharers
    outer = gathered.shape[2]
    rows = seq_count * tokens
    width = weights[0].shape[1]
    block = width // 5 if width % 640 == 0 else width
    me = (lax.axis_index("head") // 2).astype(jnp.int32).reshape(1)

    def kernel(me_ref, x_ref, *refs):
        w_refs = refs[: len(weights)]
        out_refs = refs[len(weights) : -1]
        a_ref = refs[-1]

        @pl.when(pl.program_id(0) == 0)
        def _():
            for step in range(outer):
                far = (me_ref[0] + step) % outer
                base = step * rows
                for seq in range(seq_count):
                    for near in range(len(weights)):
                        for slot in range(whole):
                            col = (seq * whole + slot) * HEAD_DIM
                            a_ref[near, base : base + rows, col : col + HEAD_DIM] = x_ref[
                                seq, near, far, slot * rows : (slot + 1) * rows, :
                            ]
                        if shared:
                            col = (whole * seq_count + seq // sharers) * HEAD_DIM
                            to = base + (seq % sharers) * part_rows * tokens
                            a_ref[
                                near, to : to + part_rows * tokens, col : col + HEAD_DIM
                            ] = x_ref[
                                seq, near, far, whole * rows : (whole * rows + part_rows * tokens), :
                            ]

        total = None
        for near, w_ref in enumerate(w_refs):
            term = jnp.dot(a_ref[near], w_ref[...], preferred_element_type=jnp.float32)
            total = term if total is None else total + term
        total = total.astype(jnp.bfloat16)
        for step, out_ref in enumerate(out_refs):
            for seq in range(seq_count):
                at = step * rows + seq * tokens
                out_ref[seq] = total[at : at + tokens]

    out = jax.ShapeDtypeStruct((seq_count, tokens, width), jnp.bfloat16)
    return pl.pallas_call(
        kernel,
        grid=(width // block,),
        in_specs=[
            pl.BlockSpec(memory_space=pltpu.SMEM),
            pl.BlockSpec(gathered.shape, lambda i: (0, 0, 0, 0, 0)),
        ]
        + [pl.BlockSpec((w.shape[0], block), lambda i: (0, i)) for w in weights],
        out_specs=[pl.BlockSpec((seq_count, tokens, block), lambda i: (0, 0, i))] * outer,
        out_shape=[out] * outer,
        scratch_shapes=[
            pltpu.VMEM((len(weights), outer * rows, group * HEAD_DIM), jnp.bfloat16)
        ],
        name="project",
    )(me, gathered, *weights)


def finish_kernel_call(columns, residual, gate, shift, scale, head_weight, head_bias):
    parts, tokens, width = columns.shape
    model = parts * width

    def kernel(y_ref, r_ref, g_ref, sh_ref, sc_ref, w_ref, b_ref, h_ref, p_ref):
        total = jnp.zeros((tokens, 1), jnp.float32)
        for i in range(parts):
            at = slice(i * width, (i + 1) * width)
            hidden = (
                r_ref[:, at].astype(jnp.float32) + g_ref[:, at] * y_ref[i].astype(jnp.float32)
            ).astype(jnp.bfloat16)
            h_ref[:, at] = hidden
            total = total + jnp.sum(hidden.astype(jnp.float32), -1, keepdims=True)
        mean = total / model
        square = jnp.zeros((tokens, 1), jnp.float32)
        for i in range(parts):
            center = h_ref[:, i * width : (i + 1) * width].astype(jnp.float32) - mean
            square = square + jnp.sum(center * center, -1, keepdims=True)
        inverse = lax.rsqrt(square / model + 1e-06)
        latent = jnp.zeros((tokens, w_ref.shape[1]), jnp.float32)
        for i in range(parts):
            at = slice(i * width, (i + 1) * width)
            center = h_ref[:, at].astype(jnp.float32) - mean
            normed = (center * inverse * (1.0 + sc_ref[:, at]) + sh_ref[:, at]).astype(jnp.bfloat16)
            latent = latent + jnp.dot(normed, w_ref[at, :], preferred_element_type=jnp.float32)
        p_ref[...] = (latent + b_ref[...]).astype(jnp.bfloat16)

    return pl.pallas_call(
        kernel,
        out_shape=(
            jax.ShapeDtypeStruct((tokens, model), jnp.bfloat16),
            jax.ShapeDtypeStruct((tokens, head_weight.shape[1]), jnp.bfloat16),
        ),
        name="finish",
    )(
        columns,
        residual,
        gate.reshape(1, -1),
        shift.reshape(1, -1),
        scale.reshape(1, -1),
        head_weight,
        head_bias.reshape(1, -1),
    )


def neighbour(value, seq_step, head_step):
    seq_count, head_count = (lax.axis_size("seq"), lax.axis_size("head"))
    pairs = []
    for seq in range(seq_count):
        for head in range(head_count):
            to_seq, to_head = (seq + seq_step, head + head_step)
            if 0 <= to_seq < seq_count and 0 <= to_head < head_count:
                pairs.append((seq * head_count + head, to_seq * head_count + to_head))
    return lax.ppermute(value, ("seq", "head"), pairs)


def swap_near(value, head_count):
    return lax.ppermute(value, "head", [(i, i ^ 1) for i in range(head_count)])


def on_device(
    queries,
    attn_keys,
    attn_values,
    residual,
    out_weight,
    out_gate,
    head_shift,
    head_scale,
    head_weight,
    head_bias,
    conv_weight,
    conv_bias,
    norm_gain,
):
    head_count, seq_count = (lax.axis_size("head"), lax.axis_size("seq"))
    frames, height, breadth, width = queries.shape
    group = width // HEAD_DIM // head_count
    shared = group % seq_count
    tokens = frames * height * breadth
    fits = (
        group >= seq_count
        and (shared == 0 or seq_count % shared == 0)
        and head_count % 2 == 0
        and height == 1
        and tokens % 16 == 0
        and frames >= 2
    )
    if not fits:
        return general_path(
            queries,
            attn_keys,
            attn_values,
            residual,
            out_weight,
            out_gate,
            head_shift,
            head_scale,
            head_weight,
            head_bias,
            conv_weight,
            conv_bias,
            norm_gain,
        )
    weights = [out_weight, swap_near(out_weight, head_count)]
    packed = pack_heads(
        queries.reshape(tokens, width),
        attn_keys.reshape(tokens, width),
        attn_values.reshape(tokens, width),
        seq_count,
        head_count,
    )
    packed = lax.all_to_all(packed, ("seq", "head"), split_axis=0, concat_axis=0, tiled=True)
    keep, send = attend_kernel_call(packed, seq_count, head_count, group)
    attended = jnp.stack([keep, swap_near(send, head_count)])
    gathered = lax.all_gather(attended, "seq", axis=0, tiled=False)
    terms = project_kernel_call(gathered, weights, seq_count, group, tokens)
    columns = terms[0].astype(jnp.float32)
    for step in range(1, head_count // 2):
        pairs = [(i, (i + 2 * step) % head_count) for i in range(head_count)]
        columns = columns + lax.ppermute(terms[step], "head", pairs).astype(jnp.float32)
    columns = columns.astype(jnp.bfloat16)
    columns = lax.all_to_all(columns, "seq", split_axis=0, concat_axis=0, tiled=True)
    hidden, latent = finish_kernel_call(
        columns,
        residual.reshape(tokens, -1),
        out_gate,
        head_shift,
        head_scale,
        head_weight,
        head_bias,
    )
    before = [neighbour(latent, step, 1) for step in (1, 0, -1)]
    now = [neighbour(latent, 1, 0), latent, neighbour(latent, -1, 0)]
    channels = latent.shape[1] // 4
    grid = jnp.stack([jnp.stack(before), jnp.stack(now)]).reshape(
        2, 3, frames, breadth, 2, 2, channels
    )
    video = grid.transpose(0, 2, 1, 4, 3, 5, 6).reshape(2 * frames, 6, 2 * breadth, channels)
    video = video[frames - 2 :, 1:5]
    padded = jnp.pad(video, ((0, 0), (0, 0), (1, 1), (0, 0)))
    features = convolve(padded, frames, conv_weight, conv_bias, norm_gain)
    return (hidden.reshape(residual.shape), features)


def solution(mesh):
    return jax.shard_map(
        on_device,
        mesh=mesh,
        in_specs=(
            P(("clip", "head"), "seq", None, None),
            P(("clip", "head"), "seq", None, None),
            P(("clip", "head"), "seq", None, None),
            P(("clip", "head"), "seq", None, None),
            P("head", "seq"),
            P(),
            P(),
            P(),
            P(),
            P(),
            P(),
            P(),
            P(),
        ),
        out_specs=(P(("clip", "head"), "seq", None, None), P(("clip", "head"), "seq", None, None)),
        check_vma=False,
    )
```

```python
import jax
import jax.numpy as jnp
from jax import lax
from jax.experimental import pallas as pl
from jax.experimental.pallas import tpu as pltpu
from jax.sharding import PartitionSpec as P

HEAD_DIM = 128


def from_behind(value, axis, steps):
    count = lax.axis_size(axis)
    first, last = (max(0, -steps), min(count, count - steps))
    return lax.ppermute(value, axis, [(source, source + steps) for source in range(first, last)])


def padded_2(x, sides, width):
    for axis, dim in sides:
        peers, length = (lax.axis_size(axis), x.shape[dim])
        up = [(i, (i + 1) % peers) for i in range(peers - 1)]
        down = [(j, i) for i, j in up]
        last = lax.slice_in_dim(x, length - width, length, axis=dim)
        first = lax.slice_in_dim(x, 0, width, axis=dim)
        before = lax.ppermute(last, axis, up)
        after = lax.ppermute(first, axis, down)
        x = jnp.concatenate([before, x, after], axis=dim)
    return x


def head_latent(hidden, head_shift, head_scale, head_weight, head_bias):
    values = hidden.astype(jnp.float32)
    center = values - jnp.mean(values, -1, keepdims=True)
    spread = jnp.mean(center * center, -1, keepdims=True)
    normed = (center * lax.rsqrt(spread + 1e-06) * (1.0 + head_scale) + head_shift).astype(
        jnp.bfloat16
    )
    flat = normed.reshape(-1, normed.shape[-1])
    latent = (jnp.dot(flat, head_weight, preferred_element_type=jnp.float32) + head_bias).astype(
        jnp.bfloat16
    )
    frames, height, breadth = (hidden.shape[0], hidden.shape[1], hidden.shape[2])
    channels = head_weight.shape[1] // 4
    patches = latent.reshape(frames, height, breadth, 2, 2, channels).transpose(0, 1, 3, 2, 4, 5)
    return patches.reshape(frames, height * 2, breadth * 2, channels)


def convolve(padded, frames, conv_weight, conv_bias, norm_gain):
    height = padded.shape[1] - 2
    breadth = padded.shape[2] - 2
    stacked = jnp.concatenate(
        [
            padded[
                time_off : time_off + frames,
                row_off : row_off + height,
                col_off : col_off + breadth,
            ]
            for time_off in range(3)
            for row_off in range(3)
            for col_off in range(3)
        ],
        -1,
    )
    kernel = conv_weight.reshape(-1, conv_weight.shape[-1])
    linear = (
        jnp.dot(stacked.reshape(-1, stacked.shape[-1]), kernel, preferred_element_type=jnp.float32)
        + conv_bias
    )
    normed = linear * lax.rsqrt(jnp.mean(linear * linear, -1, keepdims=True) + 1e-06) * norm_gain
    return jax.nn.silu(normed).astype(jnp.bfloat16).reshape(frames, height, breadth, -1)


def attend_block(carried, block_keys, block_values, query_heads):
    running, denominator, weighted = carried
    scores = jnp.einsum("hqd,khd->hqk", query_heads, block_keys, preferred_element_type=jnp.float32)
    scores = scores * query_heads.shape[-1] ** (-0.5)
    newmax = jnp.maximum(running, jnp.max(scores, -1))
    factor = jnp.exp(running - newmax)
    weights = jnp.exp(scores - newmax[..., None])
    denominator = denominator * factor + jnp.sum(weights, -1)
    product = jnp.einsum(
        "hqk,khd->hqd",
        weights.astype(jnp.bfloat16),
        block_values,
        preferred_element_type=jnp.float32,
    )
    weighted = weighted * factor[..., None] + product
    return (newmax, denominator, weighted)


def fold_pieces(query_heads, carried, pieces):
    key_piece, value_piece = pieces
    frames, height, breadth = (key_piece.shape[0], key_piece.shape[1], key_piece.shape[2])
    heads_here, head_width = (query_heads.shape[0], query_heads.shape[2])
    group_rows = 4

    def regroup(one_piece):
        shaped = one_piece.reshape(
            frames, height // group_rows, group_rows, breadth, heads_here, head_width
        )
        shaped = shaped.transpose(1, 0, 2, 3, 4, 5)
        return shaped.reshape(
            height // group_rows, frames * group_rows * breadth, heads_here, head_width
        )

    def advance(inner, blocks):
        return (attend_block(inner, blocks[0], blocks[1], query_heads), None)

    carried, _ = lax.scan(advance, carried, (regroup(key_piece), regroup(value_piece)))
    return carried


def general_path(
    queries,
    attn_keys,
    attn_values,
    residual,
    out_weight,
    out_gate,
    head_shift,
    head_scale,
    head_weight,
    head_bias,
    conv_weight,
    conv_bias,
    norm_gain,
):
    head_count = lax.axis_size("head")
    frames_dev = queries.shape[0]
    group_width = queries.shape[3] // head_count
    head_width = HEAD_DIM
    heads_here = group_width // head_width
    local_queries, local_keys, local_values = (
        lax.all_to_all(queries, "head", split_axis=3, concat_axis=0, tiled=True),
        lax.all_to_all(attn_keys, "head", split_axis=3, concat_axis=0, tiled=True),
        lax.all_to_all(attn_values, "head", split_axis=3, concat_axis=0, tiled=True),
    )
    frames_all, height, breadth = (
        local_queries.shape[0],
        local_queries.shape[1],
        local_queries.shape[2],
    )
    count = frames_all * height * breadth
    query_heads = local_queries.reshape(count, heads_here, head_width).transpose(1, 0, 2)
    initial = (
        jnp.full((heads_here, count), -1e30, jnp.float32),
        jnp.zeros((heads_here, count), jnp.float32),
        jnp.zeros((heads_here, count, head_width), jnp.float32),
    )
    carried = fold_pieces(
        query_heads,
        initial,
        (
            lax.all_gather(local_keys, "seq", axis=1, tiled=True),
            lax.all_gather(local_values, "seq", axis=1, tiled=True),
        ),
    )
    running, denominator, weighted = carried
    attended = (weighted / denominator[..., None]).astype(jnp.bfloat16)
    attended = attended.transpose(1, 0, 2).reshape(count, group_width)
    partial_value = jnp.dot(
        attended,
        lax.all_gather(out_weight, "seq", axis=1, tiled=True),
        preferred_element_type=jnp.float32,
    )
    partial_value = partial_value.reshape(frames_all, height, breadth, partial_value.shape[-1])
    owned = lax.psum_scatter(
        partial_value.astype(jnp.bfloat16), "head", scatter_dimension=0, tiled=True
    ).astype(jnp.float32)
    hidden = (residual.astype(jnp.float32) + out_gate * owned).astype(jnp.bfloat16)
    own_video = head_latent(hidden, head_shift, head_scale, head_weight, head_bias)
    earlier = from_behind(own_video, "head", 1)
    video = jnp.concatenate([earlier, own_video], 0)
    extended = padded_2(video, (("seq", 1),), 1)
    padded = jnp.pad(extended, ((0, 0), (0, 0), (1, 1), (0, 0)))
    features = convolve(padded, frames_dev, conv_weight, conv_bias, norm_gain)
    return (hidden, features)


def pack_heads(queries, keys, values, seq_count, head_count):
    tokens, width = queries.shape
    group = width // HEAD_DIM // head_count
    whole, shared = divmod(group, seq_count)
    slots = whole + (shared > 0)

    def heads_of(seq):
        owned = [seq * whole + i for i in range(whole)]
        if shared:
            owned.append(whole * seq_count + seq // (seq_count // shared))
        return owned

    def kernel(q_ref, k_ref, v_ref, out_ref):
        for seq in range(seq_count):
            for head in range(head_count):
                for slot, local in enumerate(heads_of(seq)):
                    col = (head * group + local) * HEAD_DIM
                    for part, ref in enumerate((q_ref, k_ref, v_ref)):
                        to = (slot * 3 + part) * HEAD_DIM
                        out_ref[seq * head_count + head, :, to : to + HEAD_DIM] = ref[
                            :, col : col + HEAD_DIM
                        ]

    return pl.pallas_call(
        kernel,
        out_shape=jax.ShapeDtypeStruct(
            (seq_count * head_count, tokens, slots * 3 * HEAD_DIM), queries.dtype
        ),
        name="pack_heads",
    )(queries, keys, values)


def attend_kernel_call(packed, seq_count, head_count, group):
    tokens = packed.shape[1]
    whole, shared = divmod(group, seq_count)
    sharers = seq_count // shared if shared else 1
    row = head_count * tokens
    total = seq_count * row
    part_rows = seq_count // sharers
    out_blocks = whole * seq_count + (part_rows if shared else 0)
    outer = head_count // 2
    place = jnp.stack([lax.axis_index("seq") % sharers, lax.axis_index("head") % 2])

    def kernel(place_ref, x_ref, keep_ref, send_ref, result_ref):
        def one(slot, first, rows_of_seq, base):
            at = slot * 3 * HEAD_DIM
            count = rows_of_seq * head_count
            q = x_ref[pl.ds(first, count), :, at : at + HEAD_DIM]
            q = q.reshape(count * tokens, HEAD_DIM)
            k = x_ref[:, :, at + HEAD_DIM : at + 2 * HEAD_DIM].reshape(total, HEAD_DIM)
            v = x_ref[:, :, at + 2 * HEAD_DIM : at + 3 * HEAD_DIM].reshape(total, HEAD_DIM)
            scores = lax.dot_general(
                q, k, (((1,), (1,)), ((), ())), preferred_element_type=jnp.float32
            )
            scores = scores * HEAD_DIM ** (-0.5)
            weights = jnp.exp(scores - jnp.max(scores, -1, keepdims=True))
            denominator = jnp.sum(weights, -1, keepdims=True)
            product = jnp.dot(weights.astype(jnp.bfloat16), v, preferred_element_type=jnp.float32)
            result = (product / denominator).astype(jnp.bfloat16)
            result_ref[0:count] = result.reshape(count, tokens, HEAD_DIM)
            for seq in range(rows_of_seq):
                for far in range(outer):
                    to = (base + seq) * tokens
                    mine = seq * head_count + far * 2
                    keep_ref[far, to : to + tokens, :] = result_ref[mine + place_ref[1]]
                    send_ref[far, to : to + tokens, :] = result_ref[mine + 1 - place_ref[1]]

        for slot in range(whole):
            one(slot, 0, seq_count, slot * seq_count)
        if shared:
            one(whole, place_ref[0] * part_rows * head_count, part_rows, whole * seq_count)

    half = jax.ShapeDtypeStruct((outer, out_blocks * tokens, HEAD_DIM), jnp.bfloat16)
    return pl.pallas_call(
        kernel,
        in_specs=[
            pl.BlockSpec(memory_space=pltpu.SMEM),
            pl.BlockSpec(memory_space=pltpu.VMEM),
        ],
        out_shape=(half, half),
        scratch_shapes=[pltpu.VMEM((seq_count * head_count, tokens, HEAD_DIM), jnp.bfloat16)],
        name="attend",
    )(place.astype(jnp.int32), packed)


def project_kernel_call(gathered, weights, seq_count, group, tokens, step):
    whole, shared = divmod(group, seq_count)
    sharers = seq_count // shared if shared else 1
    part_rows = seq_count // sharers
    outer = gathered.shape[2]
    rows = seq_count * tokens
    width = weights[0].shape[1]
    block = width // 5 if width % 640 == 0 else width
    far = ((lax.axis_index("head") // 2 + step) % outer).astype(jnp.int32).reshape(1)

    def kernel(far_ref, x_ref, *refs):
        w_refs, out_ref, a_ref = (refs[:-2], refs[-2], refs[-1])

        @pl.when(pl.program_id(0) == 0)
        def _():
            at = far_ref[0]
            for seq in range(seq_count):
                for near in range(len(weights)):
                    for slot in range(whole):
                        col = (seq * whole + slot) * HEAD_DIM
                        a_ref[near, :, col : col + HEAD_DIM] = x_ref[
                            seq, near, at, slot * rows : (slot + 1) * rows, :
                        ]
                    if shared:
                        col = (whole * seq_count + seq // sharers) * HEAD_DIM
                        to = (seq % sharers) * part_rows * tokens
                        a_ref[near, to : to + part_rows * tokens, col : col + HEAD_DIM] = x_ref[
                            seq, near, at, whole * rows : (whole * rows + part_rows * tokens), :
                        ]

        total = None
        for near, w_ref in enumerate(w_refs):
            term = jnp.dot(a_ref[near], w_ref[...], preferred_element_type=jnp.float32)
            total = term if total is None else total + term
        total = total.astype(jnp.bfloat16)
        for seq in range(seq_count):
            out_ref[seq] = total[seq * tokens : (seq + 1) * tokens]

    return pl.pallas_call(
        kernel,
        grid=(width // block,),
        in_specs=[
            pl.BlockSpec(memory_space=pltpu.SMEM),
            pl.BlockSpec(gathered.shape, lambda i: (0, 0, 0, 0, 0)),
        ]
        + [pl.BlockSpec((w.shape[0], block), lambda i: (0, i)) for w in weights],
        out_specs=pl.BlockSpec((seq_count, tokens, block), lambda i: (0, 0, i)),
        out_shape=jax.ShapeDtypeStruct((seq_count, tokens, width), jnp.bfloat16),
        scratch_shapes=[pltpu.VMEM((len(weights), rows, group * HEAD_DIM), jnp.bfloat16)],
        cost_estimate=pl.CostEstimate(
            flops=2 * rows * group * HEAD_DIM * len(weights) * width,
            bytes_accessed=2 * group * HEAD_DIM * len(weights) * width,
            transcendentals=0,
        ),
        name="project_far" if step else "project_near",
    )(far, gathered, *weights)


def finish_kernel_call(columns, residual, gate, shift, scale, head_weight, head_bias):
    parts, tokens, width = columns.shape
    model = parts * width

    def kernel(y_ref, r_ref, g_ref, sh_ref, sc_ref, w_ref, b_ref, h_ref, p_ref):
        total = jnp.zeros((tokens, 1), jnp.float32)
        for i in range(parts):
            at = slice(i * width, (i + 1) * width)
            hidden = (
                r_ref[:, at].astype(jnp.float32) + g_ref[:, at] * y_ref[i].astype(jnp.float32)
            ).astype(jnp.bfloat16)
            h_ref[:, at] = hidden
            total = total + jnp.sum(hidden.astype(jnp.float32), -1, keepdims=True)
        mean = total / model
        square = jnp.zeros((tokens, 1), jnp.float32)
        for i in range(parts):
            center = h_ref[:, i * width : (i + 1) * width].astype(jnp.float32) - mean
            square = square + jnp.sum(center * center, -1, keepdims=True)
        inverse = lax.rsqrt(square / model + 1e-06)
        latent = jnp.zeros((tokens, w_ref.shape[1]), jnp.float32)
        for i in range(parts):
            at = slice(i * width, (i + 1) * width)
            center = h_ref[:, at].astype(jnp.float32) - mean
            normed = (center * inverse * (1.0 + sc_ref[:, at]) + sh_ref[:, at]).astype(jnp.bfloat16)
            latent = latent + jnp.dot(normed, w_ref[at, :], preferred_element_type=jnp.float32)
        p_ref[...] = (latent + b_ref[...]).astype(jnp.bfloat16)

    return pl.pallas_call(
        kernel,
        out_shape=(
            jax.ShapeDtypeStruct((tokens, model), jnp.bfloat16),
            jax.ShapeDtypeStruct((tokens, head_weight.shape[1]), jnp.bfloat16),
        ),
        name="finish",
    )(
        columns,
        residual,
        gate.reshape(1, -1),
        shift.reshape(1, -1),
        scale.reshape(1, -1),
        head_weight,
        head_bias.reshape(1, -1),
    )


def adjacent_rows(value):
    count = lax.axis_size("seq")
    mine = lax.axis_index("seq")

    def exchange(first):
        pairs = [(i, i + 1) for i in range(first, count - 1, 2)]
        return lax.ppermute(value, "seq", pairs + [(j, i) for i, j in pairs])

    even, odd = (exchange(0), exchange(1))
    second = mine % 2 == 1
    return (jnp.where(second, even, odd), jnp.where(second, odd, even))


def swap_near(value, head_count):
    return lax.ppermute(value, "head", [(i, i ^ 1) for i in range(head_count)])


def on_device(
    queries,
    attn_keys,
    attn_values,
    residual,
    out_weight,
    out_gate,
    head_shift,
    head_scale,
    head_weight,
    head_bias,
    conv_weight,
    conv_bias,
    norm_gain,
):
    head_count, seq_count = (lax.axis_size("head"), lax.axis_size("seq"))
    frames, height, breadth, width = queries.shape
    group = width // HEAD_DIM // head_count
    shared = group % seq_count
    tokens = frames * height * breadth
    fits = (
        group >= seq_count
        and (shared == 0 or seq_count % shared == 0)
        and head_count % 2 == 0
        and height == 1
        and tokens % 16 == 0
        and frames >= 2
    )
    if not fits:
        return general_path(
            queries,
            attn_keys,
            attn_values,
            residual,
            out_weight,
            out_gate,
            head_shift,
            head_scale,
            head_weight,
            head_bias,
            conv_weight,
            conv_bias,
            norm_gain,
        )
    weights = [out_weight, swap_near(out_weight, head_count)]
    packed = pack_heads(
        queries.reshape(tokens, width),
        attn_keys.reshape(tokens, width),
        attn_values.reshape(tokens, width),
        seq_count,
        head_count,
    )
    packed = lax.all_to_all(packed, ("seq", "head"), split_axis=0, concat_axis=0, tiled=True)
    keep, send = attend_kernel_call(packed, seq_count, head_count, group)
    attended = jnp.stack([keep, swap_near(send, head_count)])
    gathered = lax.all_gather(attended, "seq", axis=0, tiled=False)
    received = []
    for step in range(1, head_count // 2):
        pairs = [(i, (i + 2 * step) % head_count) for i in range(head_count)]
        term = project_kernel_call(gathered, weights, seq_count, group, tokens, step)
        received.append(lax.ppermute(term, "head", pairs))
    columns = project_kernel_call(gathered, weights, seq_count, group, tokens, 0)
    columns = columns.astype(jnp.float32)
    for term in received:
        columns = columns + term.astype(jnp.float32)
    columns = columns.astype(jnp.bfloat16)
    columns = lax.all_to_all(columns, "seq", split_axis=0, concat_axis=0, tiled=True)
    hidden, latent = finish_kernel_call(
        columns,
        residual.reshape(tokens, -1),
        out_gate,
        head_shift,
        head_scale,
        head_weight,
        head_bias,
    )
    latent = jnp.stack([from_behind(latent, "head", 1), latent])
    above, below = adjacent_rows(latent)
    channels = latent.shape[-1] // 4
    grid = jnp.stack([above, latent, below], 1).reshape(
        2, 3, frames, breadth, 2, 2, channels
    )
    video = grid.transpose(0, 2, 1, 4, 3, 5, 6).reshape(2 * frames, 6, 2 * breadth, channels)
    video = video[frames - 2 :, 1:5]
    padded = jnp.pad(video, ((0, 0), (0, 0), (1, 1), (0, 0)))
    features = convolve(padded, frames, conv_weight, conv_bias, norm_gain)
    return (hidden.reshape(residual.shape), features)


def solution(mesh):
    return jax.shard_map(
        on_device,
        mesh=mesh,
        in_specs=(
            P(("clip", "head"), "seq", None, None),
            P(("clip", "head"), "seq", None, None),
            P(("clip", "head"), "seq", None, None),
            P(("clip", "head"), "seq", None, None),
            P("head", "seq"),
            P(),
            P(),
            P(),
            P(),
            P(),
            P(),
            P(),
            P(),
        ),
        out_specs=(P(("clip", "head"), "seq", None, None), P(("clip", "head"), "seq", None, None)),
        check_vma=False,
    )
```

```python
import jax
import jax.numpy as jnp
from jax import lax
from jax.experimental import pallas as pl
from jax.experimental.pallas import tpu as pltpu
from jax.sharding import PartitionSpec as P

HEAD_DIM = 128
KERNEL_VMEM = 24 * 2**20


def from_behind(value, axis, steps):
    count = lax.axis_size(axis)
    first, last = (max(0, -steps), min(count, count - steps))
    return lax.ppermute(value, axis, [(source, source + steps) for source in range(first, last)])


def padded_2(x, sides, width):
    for axis, dim in sides:
        peers, length = (lax.axis_size(axis), x.shape[dim])
        up = [(i, (i + 1) % peers) for i in range(peers - 1)]
        down = [(j, i) for i, j in up]
        last = lax.slice_in_dim(x, length - width, length, axis=dim)
        first = lax.slice_in_dim(x, 0, width, axis=dim)
        before = lax.ppermute(last, axis, up)
        after = lax.ppermute(first, axis, down)
        x = jnp.concatenate([before, x, after], axis=dim)
    return x


def head_latent(hidden, head_shift, head_scale, head_weight, head_bias):
    values = hidden.astype(jnp.float32)
    center = values - jnp.mean(values, -1, keepdims=True)
    spread = jnp.mean(center * center, -1, keepdims=True)
    normed = (center * lax.rsqrt(spread + 1e-06) * (1.0 + head_scale) + head_shift).astype(
        jnp.bfloat16
    )
    flat = normed.reshape(-1, normed.shape[-1])
    latent = (jnp.dot(flat, head_weight, preferred_element_type=jnp.float32) + head_bias).astype(
        jnp.bfloat16
    )
    frames, height, breadth = (hidden.shape[0], hidden.shape[1], hidden.shape[2])
    channels = head_weight.shape[1] // 4
    patches = latent.reshape(frames, height, breadth, 2, 2, channels).transpose(0, 1, 3, 2, 4, 5)
    return patches.reshape(frames, height * 2, breadth * 2, channels)


def convolve(padded, frames, conv_weight, conv_bias, norm_gain):
    height = padded.shape[1] - 2
    breadth = padded.shape[2] - 2
    stacked = jnp.concatenate(
        [
            padded[
                time_off : time_off + frames,
                row_off : row_off + height,
                col_off : col_off + breadth,
            ]
            for time_off in range(3)
            for row_off in range(3)
            for col_off in range(3)
        ],
        -1,
    )
    kernel = conv_weight.reshape(-1, conv_weight.shape[-1])
    linear = (
        jnp.dot(stacked.reshape(-1, stacked.shape[-1]), kernel, preferred_element_type=jnp.float32)
        + conv_bias
    )
    normed = linear * lax.rsqrt(jnp.mean(linear * linear, -1, keepdims=True) + 1e-06) * norm_gain
    return jax.nn.silu(normed).astype(jnp.bfloat16).reshape(frames, height, breadth, -1)


def attend_block(carried, block_keys, block_values, query_heads):
    running, denominator, weighted = carried
    scores = jnp.einsum("hqd,khd->hqk", query_heads, block_keys, preferred_element_type=jnp.float32)
    scores = scores * query_heads.shape[-1] ** (-0.5)
    newmax = jnp.maximum(running, jnp.max(scores, -1))
    factor = jnp.exp(running - newmax)
    weights = jnp.exp(scores - newmax[..., None])
    denominator = denominator * factor + jnp.sum(weights, -1)
    product = jnp.einsum(
        "hqk,khd->hqd",
        weights.astype(jnp.bfloat16),
        block_values,
        preferred_element_type=jnp.float32,
    )
    weighted = weighted * factor[..., None] + product
    return (newmax, denominator, weighted)


def fold_pieces(query_heads, carried, pieces):
    key_piece, value_piece = pieces
    frames, height, breadth = (key_piece.shape[0], key_piece.shape[1], key_piece.shape[2])
    heads_here, head_width = (query_heads.shape[0], query_heads.shape[2])
    group_rows = 4

    def regroup(one_piece):
        shaped = one_piece.reshape(
            frames, height // group_rows, group_rows, breadth, heads_here, head_width
        )
        shaped = shaped.transpose(1, 0, 2, 3, 4, 5)
        return shaped.reshape(
            height // group_rows, frames * group_rows * breadth, heads_here, head_width
        )

    def advance(inner, blocks):
        return (attend_block(inner, blocks[0], blocks[1], query_heads), None)

    carried, _ = lax.scan(advance, carried, (regroup(key_piece), regroup(value_piece)))
    return carried


def general_path(
    queries,
    attn_keys,
    attn_values,
    residual,
    out_weight,
    out_gate,
    head_shift,
    head_scale,
    head_weight,
    head_bias,
    conv_weight,
    conv_bias,
    norm_gain,
):
    head_count = lax.axis_size("head")
    frames_dev = queries.shape[0]
    group_width = queries.shape[3] // head_count
    head_width = HEAD_DIM
    heads_here = group_width // head_width
    local_queries, local_keys, local_values = (
        lax.all_to_all(queries, "head", split_axis=3, concat_axis=0, tiled=True),
        lax.all_to_all(attn_keys, "head", split_axis=3, concat_axis=0, tiled=True),
        lax.all_to_all(attn_values, "head", split_axis=3, concat_axis=0, tiled=True),
    )
    frames_all, height, breadth = (
        local_queries.shape[0],
        local_queries.shape[1],
        local_queries.shape[2],
    )
    count = frames_all * height * breadth
    query_heads = local_queries.reshape(count, heads_here, head_width).transpose(1, 0, 2)
    initial = (
        jnp.full((heads_here, count), -1e30, jnp.float32),
        jnp.zeros((heads_here, count), jnp.float32),
        jnp.zeros((heads_here, count, head_width), jnp.float32),
    )
    carried = fold_pieces(
        query_heads,
        initial,
        (
            lax.all_gather(local_keys, "seq", axis=1, tiled=True),
            lax.all_gather(local_values, "seq", axis=1, tiled=True),
        ),
    )
    running, denominator, weighted = carried
    attended = (weighted / denominator[..., None]).astype(jnp.bfloat16)
    attended = attended.transpose(1, 0, 2).reshape(count, group_width)
    partial_value = jnp.dot(
        attended,
        lax.all_gather(out_weight, "seq", axis=1, tiled=True),
        preferred_element_type=jnp.float32,
    )
    partial_value = partial_value.reshape(frames_all, height, breadth, partial_value.shape[-1])
    owned = lax.psum_scatter(
        partial_value.astype(jnp.bfloat16), "head", scatter_dimension=0, tiled=True
    ).astype(jnp.float32)
    hidden = (residual.astype(jnp.float32) + out_gate * owned).astype(jnp.bfloat16)
    own_video = head_latent(hidden, head_shift, head_scale, head_weight, head_bias)
    earlier = from_behind(own_video, "head", 1)
    video = jnp.concatenate([earlier, own_video], 0)
    extended = padded_2(video, (("seq", 1),), 1)
    padded = jnp.pad(extended, ((0, 0), (0, 0), (1, 1), (0, 0)))
    features = convolve(padded, frames_dev, conv_weight, conv_bias, norm_gain)
    return (hidden, features)


def pack_heads(queries, keys, values, seq_count, head_count):
    tokens, width = queries.shape
    group = width // HEAD_DIM // head_count
    whole, shared = divmod(group, seq_count)
    slots = whole + (shared > 0)

    def heads_of(seq):
        owned = [seq * whole + i for i in range(whole)]
        if shared:
            owned.append(whole * seq_count + seq // (seq_count // shared))
        return owned

    def kernel(q_ref, k_ref, v_ref, out_ref):
        for seq in range(seq_count):
            for head in range(head_count):
                for slot, local in enumerate(heads_of(seq)):
                    col = (head * group + local) * HEAD_DIM
                    for part, ref in enumerate((q_ref, k_ref, v_ref)):
                        to = (slot * 3 + part) * HEAD_DIM
                        out_ref[seq * head_count + head, :, to : to + HEAD_DIM] = ref[
                            :, col : col + HEAD_DIM
                        ]

    return pl.pallas_call(
        kernel,
        out_shape=jax.ShapeDtypeStruct(
            (seq_count * head_count, tokens, slots * 3 * HEAD_DIM), queries.dtype
        ),
        compiler_params=pltpu.CompilerParams(vmem_limit_bytes=KERNEL_VMEM),
        name="pack_heads",
    )(queries, keys, values)


def attend_kernel_call(packed, seq_count, head_count, group):
    tokens = packed.shape[1]
    whole, shared = divmod(group, seq_count)
    sharers = seq_count // shared if shared else 1
    row = head_count * tokens
    total = seq_count * row
    part_rows = seq_count // sharers
    out_blocks = whole * seq_count + (part_rows if shared else 0)
    outer = head_count // 2
    place = jnp.stack([lax.axis_index("seq") % sharers, lax.axis_index("head") % 2])

    def kernel(place_ref, x_ref, keep_ref, send_ref, result_ref):
        def one(slot, first, rows_of_seq, base):
            at = slot * 3 * HEAD_DIM
            count = rows_of_seq * head_count
            q = x_ref[pl.ds(first, count), :, at : at + HEAD_DIM]
            q = q.reshape(count * tokens, HEAD_DIM)
            k = x_ref[:, :, at + HEAD_DIM : at + 2 * HEAD_DIM].reshape(total, HEAD_DIM)
            v = x_ref[:, :, at + 2 * HEAD_DIM : at + 3 * HEAD_DIM].reshape(total, HEAD_DIM)
            scores = lax.dot_general(
                q, k, (((1,), (1,)), ((), ())), preferred_element_type=jnp.float32
            )
            scores = scores * HEAD_DIM ** (-0.5)
            weights = jnp.exp(scores - jnp.max(scores, -1, keepdims=True))
            denominator = jnp.sum(weights, -1, keepdims=True)
            product = jnp.dot(weights.astype(jnp.bfloat16), v, preferred_element_type=jnp.float32)
            result = (product / denominator).astype(jnp.bfloat16)
            result_ref[0:count] = result.reshape(count, tokens, HEAD_DIM)
            for seq in range(rows_of_seq):
                for far in range(outer):
                    to = (base + seq) * tokens
                    mine = seq * head_count + far * 2
                    keep_ref[far, to : to + tokens, :] = result_ref[mine + place_ref[1]]
                    send_ref[far, to : to + tokens, :] = result_ref[mine + 1 - place_ref[1]]

        for slot in range(whole):
            one(slot, 0, seq_count, slot * seq_count)
        if shared:
            one(whole, place_ref[0] * part_rows * head_count, part_rows, whole * seq_count)

    half = jax.ShapeDtypeStruct((outer, out_blocks * tokens, HEAD_DIM), jnp.bfloat16)
    return pl.pallas_call(
        kernel,
        in_specs=[
            pl.BlockSpec(memory_space=pltpu.SMEM),
            pl.BlockSpec(memory_space=pltpu.VMEM),
        ],
        out_shape=(half, half),
        scratch_shapes=[pltpu.VMEM((seq_count * head_count, tokens, HEAD_DIM), jnp.bfloat16)],
        compiler_params=pltpu.CompilerParams(vmem_limit_bytes=KERNEL_VMEM),
        name="attend",
    )(place.astype(jnp.int32), packed)


def project_kernel_call(gathered, weights, seq_count, group, tokens, step):
    whole, shared = divmod(group, seq_count)
    sharers = seq_count // shared if shared else 1
    part_rows = seq_count // sharers
    outer = gathered.shape[2]
    rows = seq_count * tokens
    width = weights[0].shape[1]
    block = width // 5 if width % 640 == 0 else width
    far = ((lax.axis_index("head") // 2 + step) % outer).astype(jnp.int32).reshape(1)

    def kernel(far_ref, x_ref, *refs):
        w_refs, out_ref, a_ref = (refs[:-2], refs[-2], refs[-1])

        at = far_ref[0]
        for seq in range(seq_count):
            for near in range(len(weights)):
                for slot in range(whole):
                    col = (seq * whole + slot) * HEAD_DIM
                    a_ref[near, :, col : col + HEAD_DIM] = x_ref[
                        seq, near, at, slot * rows : (slot + 1) * rows, :
                    ]
                if shared:
                    col = (whole * seq_count + seq // sharers) * HEAD_DIM
                    to = (seq % sharers) * part_rows * tokens
                    a_ref[near, to : to + part_rows * tokens, col : col + HEAD_DIM] = x_ref[
                        seq, near, at, whole * rows : (whole * rows + part_rows * tokens), :
                    ]

        for col in range(0, width, block):
            total = None
            for near, w_ref in enumerate(w_refs):
                term = jnp.dot(
                    a_ref[near], w_ref[:, col : col + block], preferred_element_type=jnp.float32
                )
                total = term if total is None else total + term
            total = total.astype(jnp.bfloat16)
            for seq in range(seq_count):
                out_ref[seq, :, col : col + block] = total[seq * tokens : (seq + 1) * tokens]

    return pl.pallas_call(
        kernel,
        in_specs=[pl.BlockSpec(memory_space=pltpu.SMEM)]
        + [pl.BlockSpec(memory_space=pltpu.VMEM)] * (1 + len(weights)),
        out_shape=jax.ShapeDtypeStruct((seq_count, tokens, width), jnp.bfloat16),
        scratch_shapes=[pltpu.VMEM((len(weights), rows, group * HEAD_DIM), jnp.bfloat16)],
        cost_estimate=pl.CostEstimate(
            flops=2 * rows * group * HEAD_DIM * len(weights) * width,
            bytes_accessed=2 * group * HEAD_DIM * len(weights) * width,
            transcendentals=0,
        ),
        compiler_params=pltpu.CompilerParams(vmem_limit_bytes=KERNEL_VMEM),
        name="project_far" if step else "project_near",
    )(far, gathered, *weights)


def add_terms(terms):
    def kernel(*refs):
        total = refs[0][...].astype(jnp.float32)
        for ref in refs[1:-1]:
            total = total + ref[...].astype(jnp.float32)
        refs[-1][...] = total.astype(jnp.bfloat16)

    return pl.pallas_call(
        kernel,
        out_shape=jax.ShapeDtypeStruct(terms[0].shape, jnp.bfloat16),
        compiler_params=pltpu.CompilerParams(vmem_limit_bytes=KERNEL_VMEM),
        name="add_terms",
    )(*terms)


def finish_kernel_call(columns, residual, gate, shift, scale, head_weight, head_bias):
    parts, tokens, width = columns.shape
    model = parts * width

    def kernel(y_ref, r_ref, g_ref, sh_ref, sc_ref, w_ref, b_ref, h_ref, p_ref):
        total = jnp.zeros((tokens, 1), jnp.float32)
        for i in range(parts):
            at = slice(i * width, (i + 1) * width)
            hidden = (
                r_ref[:, at].astype(jnp.float32) + g_ref[:, at] * y_ref[i].astype(jnp.float32)
            ).astype(jnp.bfloat16)
            h_ref[:, at] = hidden
            total = total + jnp.sum(hidden.astype(jnp.float32), -1, keepdims=True)
        mean = total / model
        square = jnp.zeros((tokens, 1), jnp.float32)
        for i in range(parts):
            center = h_ref[:, i * width : (i + 1) * width].astype(jnp.float32) - mean
            square = square + jnp.sum(center * center, -1, keepdims=True)
        inverse = lax.rsqrt(square / model + 1e-06)
        latent = jnp.zeros((tokens, w_ref.shape[1]), jnp.float32)
        for i in range(parts):
            at = slice(i * width, (i + 1) * width)
            center = h_ref[:, at].astype(jnp.float32) - mean
            normed = (center * inverse * (1.0 + sc_ref[:, at]) + sh_ref[:, at]).astype(jnp.bfloat16)
            latent = latent + jnp.dot(normed, w_ref[at, :], preferred_element_type=jnp.float32)
        p_ref[...] = (latent + b_ref[...]).astype(jnp.bfloat16)

    return pl.pallas_call(
        kernel,
        out_shape=(
            jax.ShapeDtypeStruct((tokens, model), jnp.bfloat16),
            jax.ShapeDtypeStruct((tokens, head_weight.shape[1]), jnp.bfloat16),
        ),
        compiler_params=pltpu.CompilerParams(vmem_limit_bytes=KERNEL_VMEM),
        name="finish",
    )(
        columns,
        residual,
        gate.reshape(1, -1),
        shift.reshape(1, -1),
        scale.reshape(1, -1),
        head_weight,
        head_bias.reshape(1, -1),
    )


def adjacent_rows(value):
    count = lax.axis_size("seq")
    mine = lax.axis_index("seq")

    def exchange(first):
        pairs = [(i, i + 1) for i in range(first, count - 1, 2)]
        return lax.ppermute(value, "seq", pairs + [(j, i) for i, j in pairs])

    even, odd = (exchange(0), exchange(1))
    second = mine % 2 == 1
    return (jnp.where(second, even, odd), jnp.where(second, odd, even))


def swap_near(value, head_count):
    return lax.ppermute(value, "head", [(i, i ^ 1) for i in range(head_count)])


def on_device(
    queries,
    attn_keys,
    attn_values,
    residual,
    out_weight,
    out_gate,
    head_shift,
    head_scale,
    head_weight,
    head_bias,
    conv_weight,
    conv_bias,
    norm_gain,
):
    head_count, seq_count = (lax.axis_size("head"), lax.axis_size("seq"))
    frames, height, breadth, width = queries.shape
    group = width // HEAD_DIM // head_count
    shared = group % seq_count
    tokens = frames * height * breadth
    fits = (
        group >= seq_count
        and (shared == 0 or seq_count % shared == 0)
        and head_count % 2 == 0
        and height == 1
        and tokens % 16 == 0
        and frames >= 2
    )
    if not fits:
        return general_path(
            queries,
            attn_keys,
            attn_values,
            residual,
            out_weight,
            out_gate,
            head_shift,
            head_scale,
            head_weight,
            head_bias,
            conv_weight,
            conv_bias,
            norm_gain,
        )
    weights = [out_weight, swap_near(out_weight, head_count)]
    packed = pack_heads(
        queries.reshape(tokens, width),
        attn_keys.reshape(tokens, width),
        attn_values.reshape(tokens, width),
        seq_count,
        head_count,
    )
    packed = lax.all_to_all(packed, ("seq", "head"), split_axis=0, concat_axis=0, tiled=True)
    keep, send = attend_kernel_call(packed, seq_count, head_count, group)
    attended = jnp.stack([keep, swap_near(send, head_count)])
    gathered = lax.all_gather(attended, "seq", axis=0, tiled=False)
    received = []
    for step in range(1, head_count // 2):
        pairs = [(i, (i + 2 * step) % head_count) for i in range(head_count)]
        term = project_kernel_call(gathered, weights, seq_count, group, tokens, step)
        received.append(lax.ppermute(term, "head", pairs))
    columns = project_kernel_call(gathered, weights, seq_count, group, tokens, 0)
    columns = add_terms([columns] + received)
    columns = lax.all_to_all(columns, "seq", split_axis=0, concat_axis=0, tiled=True)
    hidden, latent = finish_kernel_call(
        columns,
        residual.reshape(tokens, -1),
        out_gate,
        head_shift,
        head_scale,
        head_weight,
        head_bias,
    )
    latent = jnp.stack([from_behind(latent, "head", 1), latent])
    above, below = adjacent_rows(latent)
    channels = latent.shape[-1] // 4
    grid = jnp.stack([above, latent, below], 1).reshape(
        2, 3, frames, breadth, 2, 2, channels
    )
    video = grid.transpose(0, 2, 1, 4, 3, 5, 6).reshape(2 * frames, 6, 2 * breadth, channels)
    video = video[frames - 2 :, 1:5]
    padded = jnp.pad(video, ((0, 0), (0, 0), (1, 1), (0, 0)))
    features = convolve(padded, frames, conv_weight, conv_bias, norm_gain)
    return (hidden.reshape(residual.shape), features)


def solution(mesh):
    return jax.shard_map(
        on_device,
        mesh=mesh,
        in_specs=(
            P(("clip", "head"), "seq", None, None),
            P(("clip", "head"), "seq", None, None),
            P(("clip", "head"), "seq", None, None),
            P(("clip", "head"), "seq", None, None),
            P("head", "seq"),
            P(),
            P(),
            P(),
            P(),
            P(),
            P(),
            P(),
            P(),
        ),
        out_specs=(P(("clip", "head"), "seq", None, None), P(("clip", "head"), "seq", None, None)),
        check_vma=False,
    )
```
